256 devices in a mesh: rep: 4 (over y, x), tp: 32 (over z), sub: 2 (over core).
Axes of the slice: x: 2, y: 2, z: 32, core: 2. Of those that a mesh axis runs over, the one named last changes fastest.
The devices are a block of a 4x8x32 slice.
Arguments:
- attention: bfloat16 [2048, 8192], P('rep', ('tp', 'sub')), parts along dimension 0, may hold values from -6 to 6
- out_weight: bfloat16 [8192, 8192], P(('tp', 'sub')), may hold values from -0.1875 to 0.1875
- residual: bfloat16 [2048, 8192], P('rep', ('tp', 'sub')), parts along dimension 0, may hold values from -6 to 6
- norm_gain: bfloat16 [8192], P(('tp', 'sub')), may hold values from 0.25 to 1.75
Outputs:
- quantized: bfloat16 [2048, 8192], P('rep'), parts along dimension 0
- scales: bfloat16 [2048, 64], P('rep'), parts along dimension 0
- new_residual: bfloat16 [2048, 8192], P('rep', ('tp', 'sub')), parts along dimension 0
The draws below stay inside these ranges and needn't reach their ends.
There are 4 independent parts, one for each index of `rep`. The reference program is written for one: setup_inputs(seed, part) draws one part's arguments, and reference() takes and returns one part's arrays. A program takes and returns all parts, laid end to end along the dimension named above; an argument that names none is the same for every part. Nothing has to cross between parts.
All inputs are finite; a program needn't handle non-finite values.
Results may differ from the reference program's by a relative error of at most 0.0048.
Values may be sent and summed in bfloat16 or wider, within the bound.
No kernel may reach another device: no remote copies, remote signals or barrier semaphores. Data moves between devices by JAX's collectives and lax.ppermute only.
A program may use at most 128 MiB of HBM per device.

```python
import jax
import jax.numpy as jnp
from jax import lax

D = 8192
BLOCK = 128
ROWS = 512


def with_spikes(drawn, own_key, source, target, shards_of, factor):
    owner, partner = [(jnp.arange(drawn.shape[position]) // (drawn.shape[position] // shards_of)).reshape([-1 if axis == position else 1 for axis in range(drawn.ndim)]) for position in (source, target)]
    chosen = jax.random.permutation(own_key, shards_of)[partner]
    strong = (owner == chosen) | (owner == (partner + shards_of // 2) % shards_of)
    return jnp.where(strong, factor * drawn, drawn)


def block_scale(stream_key, shape, split, low, top_value):
    def one(dim, parts):
        steps = jax.random.uniform(jax.random.fold_in(jax.random.fold_in(stream_key, 6), dim), (parts,), jnp.float32, low / len(split), top_value / len(split))
        return jnp.repeat(jnp.exp(steps), shape[dim] // parts).reshape((-1,) + (1,) * (len(shape) - dim - 1))

    loudness = one(*split[0])
    for cut in split[1:]:
        loudness = loudness * one(*cut)
    return loudness


def gaussian(own_key, shape, width, most, pieces=(), dtype=jnp.bfloat16):
    array = width * jax.random.normal(own_key, shape, jnp.float32)
    if pieces:
        array = array * block_scale(own_key, shape, pieces, -0.22, 0.18)
    return jnp.clip(array, -most, most).astype(dtype)


def heavy_noise(own_key, shape, scale, limit, split, heavy, kind=jnp.bfloat16):
    entries = scale * jax.random.normal(own_key, shape, jnp.float32)
    if split:
        entries = entries * block_scale(own_key, shape, split, -0.22, 0.18)
    return jnp.clip(with_spikes(entries, jax.random.fold_in(own_key, 3), *heavy), -limit, limit).astype(kind)


def setup_inputs(seed: int = 0, part: int = 0) -> dict:
    key_of = jax.random.split(jax.random.key(seed), 5)
    own_keys = jax.random.split(jax.random.fold_in(key_of[4], part), 5)
    return {
        "attention": gaussian(own_keys[0], (ROWS, D), 1.0, 6.0, ((1, 64),)),
        "out_weight": heavy_noise(key_of[1], (D, D), D ** -0.5, 0.1875, ((0, 64),), (0, 1, 64, 4.0)),
        "residual": gaussian(own_keys[2], (ROWS, D), 1.0, 6.0, ((1, 64),)),
        "norm_gain": jnp.clip(1.0 + 0.15 * jax.random.normal(key_of[3], (D,), jnp.float32), 0.25, 1.75).astype(jnp.bfloat16),
    }


epsilon = 0.1
floor_scale = 0.5

def reference(attention, out_weight, residual, norm_gain):
    projected = jnp.dot(attention, out_weight, preferred_element_type=jnp.float32)
    hidden = residual.astype(jnp.float32) + projected
    new_residual = hidden.astype(jnp.bfloat16)
    mean_square = lax.optimization_barrier(jnp.mean(hidden * hidden, axis=1, keepdims=True))
    normed = hidden * lax.rsqrt(mean_square + epsilon) * norm_gain.astype(jnp.float32)
    blocks = normed.reshape(hidden.shape[0], hidden.shape[1] // BLOCK, BLOCK)
    largest = lax.optimization_barrier(jnp.max(jnp.abs(blocks), axis=2))
    scales = jnp.maximum(largest, floor_scale).astype(jnp.bfloat16)
    quantized = (blocks / scales.astype(jnp.float32)[:, :, None]).reshape(hidden.shape).astype(jnp.bfloat16)
    return (quantized, scales, new_residual)
```

```python
import functools

import jax
import jax.numpy as jnp
from jax import lax
from jax.experimental import pallas as pl
from jax.experimental.pallas import tpu as pltpu
from jax.sharding import PartitionSpec as P

BLOCK = 128
epsilon = 0.1
floor_scale = 0.5
f32, f16, bf16 = jnp.float32, jnp.float16, jnp.bfloat16
sum_up = 4.0
quant_up = 2.0**14
STREAMS = 2


def arrange_kernel(chip_rows, order_ref, att_ref, res_ref, mine_ref, theirs_ref):
    n = mine_ref.shape[0] // chip_rows
    k = att_ref.shape[1]
    for out, base in ((mine_ref, 0), (theirs_ref, n)):
        for i in range(n):
            at = pl.multiple_of(order_ref[base + i], chip_rows)
            to = pl.ds(i * chip_rows, chip_rows)
            out[to, :k] = att_ref[pl.ds(at, chip_rows), :]
            out[to, k:] = res_ref[pl.ds(at, chip_rows), :]


def arrange(order, attention, residual, chip_rows):
    rows, k = attention.shape
    shape = jax.ShapeDtypeStruct((rows // 2, 2 * k), attention.dtype)
    return pl.pallas_call(
        functools.partial(arrange_kernel, chip_rows),
        in_specs=[pl.BlockSpec(memory_space=pltpu.SMEM)] + [pl.BlockSpec(memory_space=pltpu.VMEM)] * 2,
        out_specs=[pl.BlockSpec(memory_space=pltpu.VMEM)] * 2,
        out_shape=[shape, shape],
        compiler_params=pltpu.CompilerParams(vmem_limit_bytes=4 * 2**20),
    )(order, attention, residual)


COLS = 1024


def terms_kernel(chip_rows, place_ref, mine_ref, other_ref, w_ref, w_other_ref, *outs):
    k = w_ref.shape[0]
    chip_w = 2 * k
    d, s = place_ref[0], place_ref[1]
    step = pl.program_id(0)
    rows = mine_ref.shape[0]
    total = jnp.dot(mine_ref[:, :k], w_ref[...], preferred_element_type=f32)
    total += jnp.dot(other_ref[:, :k], w_other_ref[...], preferred_element_type=f32)
    total *= sum_up
    for i, out in enumerate(outs):
        out[...] = total[i * chip_rows : (i + 1) * chip_rows]

    per = COLS // chip_w
    for j in range(per):
        @pl.when(step * per + j == d)
        def _():
            a, b = mine_ref[:, k:].astype(f32) * sum_up, other_ref[:, k:].astype(f32) * sum_up
            first, second = jnp.where(s == 0, a, b), jnp.where(s == 0, b, a)
            for i, out in enumerate(outs):
                at = slice(i * chip_rows, (i + 1) * chip_rows)
                out[:, j * chip_w : j * chip_w + k] += first[at]
                out[:, j * chip_w + k : (j + 1) * chip_w] += second[at]


def terms(place, mine, other, w, w_other, chip_rows):
    width = w.shape[1]
    n = mine.shape[0] // chip_rows
    whole = pl.BlockSpec(mine.shape, lambda i: (0, 0))
    weights = pl.BlockSpec((w.shape[0], COLS), lambda i: (0, i))
    return pl.pallas_call(
        functools.partial(terms_kernel, chip_rows),
        grid=(width // COLS,),
        in_specs=[pl.BlockSpec(memory_space=pltpu.SMEM), whole, whole, weights, weights],
        out_specs=[pl.BlockSpec((chip_rows, COLS), lambda i: (0, i))] * n,
        out_shape=[OUT((chip_rows, width), f32)] * n,
        compiler_params=pltpu.CompilerParams(vmem_limit_bytes=16 * 2**20),
        cost_estimate=pl.CostEstimate(flops=4 * mine.shape[0] * w.shape[0] * width, bytes_accessed=12 * 2**20, transcendentals=0),
    )(place, mine, other, w, w_other)


OUT = jax.ShapeDtypeStruct


def per_device(attention, out_weight, residual, norm_gain):
    tp, sub = lax.axis_size("tp"), lax.axis_size("sub")
    d, s = lax.axis_index("tp"), lax.axis_index("sub")
    rows, width = attention.shape[0], out_weight.shape[1]
    chip_rows = rows // tp
    half = tp // 2
    swap = [(i, 1 - i) for i in range(sub)]
    up = [(sub * i, sub * ((i + 1) % tp)) for i in range(tp)]
    down = [(sub * i + 1, sub * ((i - 1) % tp) + 1) for i in range(tp)]

    slot = jnp.arange(half, dtype=jnp.int32)
    ahead = lax.rem(d + half - slot, tp)
    behind = jnp.where(slot == 0, d, lax.rem(d + half + slot, tp))
    order = jnp.where(s == 0, jnp.stack([ahead, behind]), jnp.stack([behind, ahead])) * chip_rows

    mine, theirs = arrange(order.reshape(-1), attention, residual, chip_rows)
    w_other = lax.ppermute(out_weight, "sub", swap)
    other = lax.ppermute(theirs, "sub", swap)
    gain_other = lax.ppermute(norm_gain, "sub", swap)
    term = terms(jnp.stack([d, s]), mine, other, out_weight, w_other, chip_rows)

    gain_pair = jnp.where(s == 0, jnp.concatenate([norm_gain, gain_other]), jnp.concatenate([gain_other, norm_gain]))
    chip_w = gain_pair.shape[0]
    gain_w = width // chip_rows
    per_row = gain_w // chip_w
    pos_r = lax.broadcasted_iota(jnp.int32, (chip_rows, gain_w), 0)
    pos_c = lax.broadcasted_iota(jnp.int32, (chip_rows, gain_w), 1)
    at_own = pos_r * per_row + pos_c // chip_w == d
    gain_tile = jnp.where(at_own, jnp.tile(gain_pair, (per_row,)).astype(f32)[None, :], 0.0).astype(f16)

    st_w = width // STREAMS

    def block(i, st):
        return term[i][:, st * st_w : (st + 1) * st_w]

    pairs = [*up, *down]
    cur = [block(0, st).astype(f16) for st in range(STREAMS)]
    cur_g = gain_tile
    for hop in range(half):
        links = up if hop == 0 else pairs
        for st in range(STREAMS):
            x = cur[st]
            if st == STREAMS - 1:
                x = jnp.concatenate([x, cur_g], 1)
            got = lax.ppermute(x, ("tp", "sub"), links).astype(f32)
            if st == STREAMS - 1:
                got_g = got[:, st_w:]
                got = got[:, :st_w]
                if hop == half - 1:
                    cur_g = jnp.where(s == 0, got_g, got_g + gain_tile.astype(f32)).astype(f16)
                else:
                    cur_g = (got_g + gain_tile.astype(f32)).astype(f16)
            if hop < half - 1:
                cur[st] = (got + block(hop + 1, st)).astype(f16)
            else:
                cur[st] = jnp.where(s == 0, got, got + block(0, st))
    whole = jnp.concatenate(cur, 1)
    own_rows = chip_rows // sub
    keep = lax.dynamic_slice_in_dim(whole, s * own_rows, own_rows, 0)
    give = lax.dynamic_slice_in_dim(whole, (1 - s) * own_rows, own_rows, 0).astype(f16)
    hidden = (keep + lax.ppermute(give, "sub", swap).astype(f32)) * (1.0 / sum_up)
    gain_all = (cur_g.astype(f32) + lax.ppermute(cur_g, "sub", swap).astype(f32)).reshape(1, width)

    mean_square = jnp.sum(hidden * hidden, axis=1, keepdims=True) / width
    normed = hidden * lax.rsqrt(mean_square + epsilon) * gain_all
    blocks = normed.reshape(own_rows, width // BLOCK, BLOCK)
    scales = jnp.maximum(jnp.max(jnp.abs(blocks), axis=2), floor_scale).astype(bf16)
    quantized = (blocks / scales.astype(f32)[:, :, None]).reshape(own_rows, width).astype(bf16)
    root = jnp.sqrt(mean_square + epsilon)
    hi = root.astype(f16)
    lo = (root - hi.astype(f32)).astype(f16)
    nb = scales.shape[1]
    small = jnp.concatenate([scales.astype(f16), hi, lo, jnp.zeros((own_rows, BLOCK - 2 - nb), f16)], 1)
    sent = jnp.concatenate([(quantized.astype(f32) * quant_up).astype(f16), small], 1)

    full = lax.all_gather(sent, ("tp", "sub"), axis=0, tiled=True)
    small_all = full[:, width:].astype(f32)
    full_quant = (full[:, :width].astype(f32) * (1.0 / quant_up)).astype(bf16)
    full_scales = small_all[:, :nb].astype(bf16)
    root_all = small_all[:, nb : nb + 1] + small_all[:, nb + 1 : nb + 2]
    me = d * sub + s
    q_own = lax.dynamic_slice_in_dim(full, me * BLOCK, BLOCK, 1).astype(f32) * (1.0 / quant_up)
    s_own = lax.dynamic_slice_in_dim(small_all, me, 1, 1)
    new_residual = (q_own * (s_own * root_all) / norm_gain.astype(f32)[None, :]).astype(bf16)
    return full_quant, full_scales, new_residual


def solution(mesh):
    in_specs = (
        P("rep", ("tp", "sub")),
        P(("tp", "sub"), None),
        P("rep", ("tp", "sub")),
        P(("tp", "sub")),
    )
    out_specs = (P("rep", None), P("rep", None), P("rep", ("tp", "sub")))
    return jax.shard_map(
        per_device, mesh=mesh, in_specs=in_specs, out_specs=out_specs, check_vma=False
    )
```

```python
import functools

import jax
import jax.numpy as jnp
from jax import lax
from jax.experimental import pallas as pl
from jax.experimental.pallas import tpu as pltpu
from jax.sharding import PartitionSpec as P

BLOCK = 128
epsilon = 0.1
floor_scale = 0.5
f32, f16, bf16 = jnp.float32, jnp.float16, jnp.bfloat16
sum_up = 4.0
quant_up = 2.0**14
STREAMS = 2


def arrange_kernel(chip_rows, order_ref, att_ref, res_ref, mine_ref, theirs_ref):
    n = mine_ref.shape[0] // chip_rows
    k = att_ref.shape[1]
    for out, base in ((mine_ref, 0), (theirs_ref, n)):
        for i in range(n):
            at = pl.multiple_of(order_ref[base + i], chip_rows)
            to = pl.ds(i * chip_rows, chip_rows)
            out[to, :k] = att_ref[pl.ds(at, chip_rows), :]
            out[to, k:] = res_ref[pl.ds(at, chip_rows), :]


def arrange(order, attention, residual, chip_rows):
    rows, k = attention.shape
    shape = jax.ShapeDtypeStruct((rows // 2, 2 * k), attention.dtype)
    return pl.pallas_call(
        functools.partial(arrange_kernel, chip_rows),
        in_specs=[pl.BlockSpec(memory_space=pltpu.SMEM)] + [pl.BlockSpec(memory_space=pltpu.VMEM)] * 2,
        out_specs=[pl.BlockSpec(memory_space=pltpu.VMEM)] * 2,
        out_shape=[shape, shape],
        compiler_params=pltpu.CompilerParams(vmem_limit_bytes=4 * 2**20),
    )(order, attention, residual)


COLS = 512


def terms_kernel(chip_rows, place_ref, mine_ref, other_ref, *refs):
    ws, w_others, outs = refs[:STREAMS], refs[STREAMS : 2 * STREAMS], refs[2 * STREAMS :]
    k = ws[0].shape[0]
    chip_w = 2 * k
    d, s = place_ref[0], place_ref[1]
    step = pl.program_id(0)
    rows = mine_ref.shape[0]
    n = rows // chip_rows
    per = COLS // chip_w
    steps = pl.num_programs(0)
    for st in range(STREAMS):
        total = jnp.dot(mine_ref[:, :k], ws[st][...], preferred_element_type=f32)
        total += jnp.dot(other_ref[:, :k], w_others[st][...], preferred_element_type=f32)
        total *= sum_up
        for i in range(n):
            outs[st * n + i][...] = total[i * chip_rows : (i + 1) * chip_rows]
        for j in range(per):
            @pl.when((st * steps + step) * per + j == d)
            def _():
                a, b = mine_ref[:, k:].astype(f32) * sum_up, other_ref[:, k:].astype(f32) * sum_up
                first, second = jnp.where(s == 0, a, b), jnp.where(s == 0, b, a)
                for i in range(n):
                    at = slice(i * chip_rows, (i + 1) * chip_rows)
                    outs[st * n + i][:, j * chip_w : j * chip_w + k] += first[at]
                    outs[st * n + i][:, j * chip_w + k : (j + 1) * chip_w] += second[at]


def terms(place, mine, other, w, w_other, chip_rows):
    width = w.shape[1]
    n = mine.shape[0] // chip_rows
    whole = pl.BlockSpec(mine.shape, lambda i: (0, 0))
    steps = width // (STREAMS * COLS)
    weights = [pl.BlockSpec((w.shape[0], COLS), lambda i, st=st: (0, st * steps + i)) for st in range(STREAMS)]
    return pl.pallas_call(
        functools.partial(terms_kernel, chip_rows),
        grid=(steps,),
        in_specs=[pl.BlockSpec(memory_space=pltpu.SMEM), whole, whole, *weights, *weights],
        out_specs=[pl.BlockSpec((chip_rows, COLS), lambda i: (0, i))] * (n * STREAMS),
        out_shape=[jax.ShapeDtypeStruct((chip_rows, width // STREAMS), f32)] * (n * STREAMS),
        compiler_params=pltpu.CompilerParams(vmem_limit_bytes=16 * 2**20),
        cost_estimate=pl.CostEstimate(flops=4 * mine.shape[0] * w.shape[0] * width, bytes_accessed=12 * 2**20, transcendentals=0),
    )(place, mine, other, *[w] * STREAMS, *[w_other] * STREAMS)


def per_device(attention, out_weight, residual, norm_gain):
    tp, sub = lax.axis_size("tp"), lax.axis_size("sub")
    d, s = lax.axis_index("tp"), lax.axis_index("sub")
    rows, width = attention.shape[0], out_weight.shape[1]
    chip_rows = rows // tp
    half = tp // 2
    swap = [(i, 1 - i) for i in range(sub)]
    up = [(sub * i, sub * ((i + 1) % tp)) for i in range(tp)]
    down = [(sub * i + 1, sub * ((i - 1) % tp) + 1) for i in range(tp)]

    slot = jnp.arange(half, dtype=jnp.int32)
    ahead = lax.rem(d + half - slot, tp)
    behind = jnp.where(slot == 0, d, lax.rem(d + half + slot, tp))
    order = jnp.where(s == 0, jnp.stack([ahead, behind]), jnp.stack([behind, ahead])) * chip_rows

    mine, theirs = arrange(order.reshape(-1), attention, residual, chip_rows)
    w_other = lax.ppermute(out_weight, "sub", swap)
    other = lax.ppermute(theirs, "sub", swap)
    gain_other = lax.ppermute(norm_gain, "sub", swap)
    term = terms(jnp.stack([d, s]), mine, other, out_weight, w_other, chip_rows)

    gain_pair = jnp.where(s == 0, jnp.concatenate([norm_gain, gain_other]), jnp.concatenate([gain_other, norm_gain]))
    chip_w = gain_pair.shape[0]
    gain_w = width // chip_rows
    per_row = gain_w // chip_w
    pos_r = lax.broadcasted_iota(jnp.int32, (chip_rows, gain_w), 0)
    pos_c = lax.broadcasted_iota(jnp.int32, (chip_rows, gain_w), 1)
    at_own = pos_r * per_row + pos_c // chip_w == d
    gain_tile = jnp.where(at_own, jnp.tile(gain_pair, (per_row,)).astype(f32)[None, :], 0.0).astype(f16)

    st_w = width // STREAMS

    def block(i, st):
        return term[st * half + i]

    pairs = [*up, *down]
    cur = [block(0, st).astype(f16) for st in range(STREAMS)]
    cur_g = gain_tile
    for hop in range(half):
        links = up if hop == 0 else pairs
        for st in range(STREAMS):
            x = cur[st]
            if st == STREAMS - 1:
                x = jnp.concatenate([x, cur_g], 1)
            got = lax.ppermute(x, ("tp", "sub"), links).astype(f32)
            if st == STREAMS - 1:
                got_g = got[:, st_w:]
                got = got[:, :st_w]
                if hop == half - 1:
                    cur_g = jnp.where(s == 0, got_g, got_g + gain_tile.astype(f32)).astype(f16)
                else:
                    cur_g = (got_g + gain_tile.astype(f32)).astype(f16)
            if hop < half - 1:
                cur[st] = (got + block(hop + 1, st)).astype(f16)
            else:
                cur[st] = jnp.where(s == 0, got, got + block(0, st))
    whole = jnp.concatenate(cur, 1)
    own_rows = chip_rows // sub
    keep = lax.dynamic_slice_in_dim(whole, s * own_rows, own_rows, 0)
    give = lax.dynamic_slice_in_dim(whole, (1 - s) * own_rows, own_rows, 0).astype(f16)
    hidden = (keep + lax.ppermute(give, "sub", swap).astype(f32)) * (1.0 / sum_up)
    gain_all = (cur_g.astype(f32) + lax.ppermute(cur_g, "sub", swap).astype(f32)).reshape(1, width)

    mean_square = jnp.sum(hidden * hidden, axis=1, keepdims=True) / width
    normed = hidden * lax.rsqrt(mean_square + epsilon) * gain_all
    blocks = normed.reshape(own_rows, width // BLOCK, BLOCK)
    scales = jnp.maximum(jnp.max(jnp.abs(blocks), axis=2), floor_scale).astype(bf16)
    quantized = (blocks / scales.astype(f32)[:, :, None]).reshape(own_rows, width).astype(bf16)
    root = jnp.sqrt(mean_square + epsilon)
    hi = root.astype(f16)
    lo = (root - hi.astype(f32)).astype(f16)
    nb = scales.shape[1]
    small = jnp.concatenate([scales.astype(f16), hi, lo, jnp.zeros((own_rows, BLOCK - 2 - nb), f16)], 1)
    sent = jnp.concatenate([(quantized.astype(f32) * quant_up).astype(f16), small], 1)

    full = lax.all_gather(sent, ("tp", "sub"), axis=0, tiled=True)
    small_all = full[:, width:].astype(f32)
    full_quant = (full[:, :width].astype(f32) * (1.0 / quant_up)).astype(bf16)
    full_scales = small_all[:, :nb].astype(bf16)
    root_all = small_all[:, nb : nb + 1] + small_all[:, nb + 1 : nb + 2]
    me = d * sub + s
    q_own = lax.dynamic_slice_in_dim(full, me * BLOCK, BLOCK, 1).astype(f32) * (1.0 / quant_up)
    s_own = lax.dynamic_slice_in_dim(small_all, me, 1, 1)
    new_residual = (q_own * (s_own * root_all) / norm_gain.astype(f32)[None, :]).astype(bf16)
    return full_quant, full_scales, new_residual


def solution(mesh):
    in_specs = (
        P("rep", ("tp", "sub")),
        P(("tp", "sub"), None),
        P("rep", ("tp", "sub")),
        P(("tp", "sub")),
    )
    out_specs = (P("rep", None), P("rep", None), P("rep", ("tp", "sub")))
    return jax.shard_map(
        per_device, mesh=mesh, in_specs=in_specs, out_specs=out_specs, check_vma=False
    )
```

```python
import functools

import jax
import jax.numpy as jnp
from jax import lax
from jax.experimental import pallas as pl
from jax.experimental.pallas import tpu as pltpu
from jax.sharding import PartitionSpec as P

BLOCK = 128
epsilon = 0.1
floor_scale = 0.5
f32, f16, bf16 = jnp.float32, jnp.float16, jnp.bfloat16
sum_up = 4.0
quant_up = 2.0**14
STREAMS = 2
JUMP = 7


def arrange_kernel(chip_rows, order_ref, att_ref, res_ref, mine_ref, theirs_ref):
    n = mine_ref.shape[0] // chip_rows
    k = att_ref.shape[1]
    for out, base in ((mine_ref, 0), (theirs_ref, n)):
        for i in range(n):
            at = pl.multiple_of(order_ref[base + i], chip_rows)
            to = pl.ds(i * chip_rows, chip_rows)
            out[to, :k] = att_ref[pl.ds(at, chip_rows), :]
            out[to, k:] = res_ref[pl.ds(at, chip_rows), :]


def arrange(order, attention, residual, chip_rows):
    rows, k = attention.shape
    shape = jax.ShapeDtypeStruct((rows // 2, 2 * k), attention.dtype)
    return pl.pallas_call(
        functools.partial(arrange_kernel, chip_rows),
        in_specs=[pl.BlockSpec(memory_space=pltpu.SMEM)] + [pl.BlockSpec(memory_space=pltpu.VMEM)] * 2,
        out_specs=[pl.BlockSpec(memory_space=pltpu.VMEM)] * 2,
        out_shape=[shape, shape],
        compiler_params=pltpu.CompilerParams(vmem_limit_bytes=4 * 2**20),
    )(order, attention, residual)


def terms_kernel(chip_rows, first_step, steps, with_gain, place_ref, mine_ref, other_ref, gain_ref, w_ref, w_other_ref, *outs):
    k, cols = w_ref.shape
    chip_w = 2 * k
    d, s = place_ref[0], place_ref[1]
    step = pl.program_id(0)

    @pl.when(step < steps)
    def _():
        total = jnp.dot(mine_ref[:, :k], w_ref[...], preferred_element_type=f32)
        total += jnp.dot(other_ref[:, :k], w_other_ref[...], preferred_element_type=f32)
        total *= sum_up
        for i, out in enumerate(outs):
            out[...] = total[i * chip_rows : (i + 1) * chip_rows]

        per = cols // chip_w
        for j in range(per):
            @pl.when((first_step + step) * per + j == d)
            def _():
                a, b = mine_ref[:, k:].astype(f32) * sum_up, other_ref[:, k:].astype(f32) * sum_up
                first, second = jnp.where(s == 0, a, b), jnp.where(s == 0, b, a)
                for i, out in enumerate(outs):
                    at = slice(i * chip_rows, (i + 1) * chip_rows)
                    out[:, j * chip_w : j * chip_w + k] += first[at]
                    out[:, j * chip_w + k : (j + 1) * chip_w] += second[at]

    if with_gain:
        @pl.when(step == steps)
        def _():
            for out in outs:
                out[...] = gain_ref[...]


def terms(place, mine, other, gain, w, w_other, chip_rows, st, with_gain):
    width = w.shape[1] // STREAMS
    n = mine.shape[0] // chip_rows
    cols = gain.shape[1] * (1 if with_gain else 2)
    steps = width // cols
    extra = 1 if with_gain else 0
    whole = pl.BlockSpec(mine.shape, lambda i: (0, 0))
    weights = pl.BlockSpec((w.shape[0], cols), lambda i: (0, st * steps + jnp.minimum(i, steps - 1)))
    return pl.pallas_call(
        functools.partial(terms_kernel, chip_rows, st * steps, steps, with_gain),
        grid=(steps + extra,),
        in_specs=[
            pl.BlockSpec(memory_space=pltpu.SMEM), whole, whole,
            pl.BlockSpec(gain.shape, lambda i: (0, 0)), weights, weights,
        ],
        out_specs=[pl.BlockSpec((chip_rows, cols), lambda i: (0, i))] * n,
        out_shape=[jax.ShapeDtypeStruct((chip_rows, width + extra * cols), f32)] * n,
        compiler_params=pltpu.CompilerParams(vmem_limit_bytes=16 * 2**20),
        cost_estimate=pl.CostEstimate(
            flops=4 * mine.shape[0] * w.shape[0] * width, bytes_accessed=6 * 2**20, transcendentals=0
        ),
    )(place, mine, other, gain, w, w_other)


def per_device(attention, out_weight, residual, norm_gain):
    tp, sub = lax.axis_size("tp"), lax.axis_size("sub")
    d, s = lax.axis_index("tp"), lax.axis_index("sub")
    rows, width = attention.shape[0], out_weight.shape[1]
    chip_rows = rows // tp
    half = tp // 2
    swap = [(i, 1 - i) for i in range(sub)]
    up = [(sub * i, sub * ((i + 1) % tp)) for i in range(tp)]
    down = [(sub * i + 1, sub * ((i - 1) % tp) + 1) for i in range(tp)]

    slot = jnp.arange(half, dtype=jnp.int32)
    ahead = lax.rem(d + half - slot, tp)
    behind = jnp.where(slot == 0, d, lax.rem(d + half + slot, tp))
    order = jnp.where(s == 0, jnp.stack([ahead, behind]), jnp.stack([behind, ahead])) * chip_rows

    mine, theirs = arrange(order.reshape(-1), attention, residual, chip_rows)
    w_other = lax.ppermute(out_weight, "sub", swap)
    other = lax.ppermute(theirs, "sub", swap)
    gain_other = lax.ppermute(norm_gain, "sub", swap)
    gain_pair = jnp.where(s == 0, jnp.concatenate([norm_gain, gain_other]), jnp.concatenate([gain_other, norm_gain]))
    chip_w = gain_pair.shape[0]
    gain_w = width // chip_rows
    per_row = gain_w // chip_w
    pos_r = lax.broadcasted_iota(jnp.int32, (chip_rows, gain_w), 0)
    pos_c = lax.broadcasted_iota(jnp.int32, (chip_rows, gain_w), 1)
    at_own = pos_r * per_row + pos_c // chip_w == d
    gain_tile = jnp.where(at_own, jnp.tile(gain_pair, (per_row,)).astype(f32)[None, :], 0.0)

    place = jnp.stack([d, s])
    term = [
        terms(place, mine, other, gain_tile, out_weight, w_other, chip_rows, st, st == STREAMS - 1)
        for st in range(STREAMS)
    ]

    st_w = width // STREAMS
    far_up = [(sub * i, sub * ((i + JUMP) % tp)) for i in range(tp)]
    far_down = [(sub * i + 1, sub * ((i - JUMP) % tp) + 1) for i in range(tp)]
    pairs = [*up, *down]
    far_pairs = [*far_up, *far_down]

    class Chain:
        def __init__(self, st, first, last, links):
            self.st, self.at, self.last, self.links = st, first, last, links
            self.value = self.add(None)

        def add(self, got):
            own = term[self.st][self.at]
            return (own if got is None else got.astype(f32) + own).astype(f16)

        def step(self):
            done = self.at == self.last
            links = self.links if done else up if self.at == 0 else pairs
            got = lax.ppermute(self.value, ("tp", "sub"), links)
            if done:
                return got
            self.at += 1
            self.value = self.add(got)

    split = half - JUMP
    chains = [Chain(st, 0, split, far_pairs) for st in range(STREAMS)]
    chains += [Chain(st, split + 1, half - 1, pairs) for st in range(STREAMS)]
    ended = {}
    while len(ended) < len(chains):
        for i, chain in enumerate(chains):
            if i not in ended and (got := chain.step()) is not None:
                ended[i] = got.astype(f32)
    cur = []
    for st in range(STREAMS):
        both = ended[st] + ended[STREAMS + st]
        cur.append(jnp.where(s == 0, both, both + term[st][0]))
    cur_g = cur[-1][:, st_w:].astype(f16)
    cur[-1] = cur[-1][:, :st_w]
    whole = jnp.concatenate(cur, 1)
    own_rows = chip_rows // sub
    keep = lax.dynamic_slice_in_dim(whole, s * own_rows, own_rows, 0)
    give = lax.dynamic_slice_in_dim(whole, (1 - s) * own_rows, own_rows, 0).astype(f16)
    hidden = (keep + lax.ppermute(give, "sub", swap).astype(f32)) * (1.0 / sum_up)
    gain_all = (cur_g.astype(f32) + lax.ppermute(cur_g, "sub", swap).astype(f32)).reshape(1, width)

    mean_square = jnp.sum(hidden * hidden, axis=1, keepdims=True) / width
    normed = hidden * lax.rsqrt(mean_square + epsilon) * gain_all
    blocks = normed.reshape(own_rows, width // BLOCK, BLOCK)
    scales = jnp.maximum(jnp.max(jnp.abs(blocks), axis=2), floor_scale).astype(bf16)
    quantized = (blocks / scales.astype(f32)[:, :, None]).reshape(own_rows, width).astype(bf16)
    root = jnp.sqrt(mean_square + epsilon)
    hi = root.astype(f16)
    lo = (root - hi.astype(f32)).astype(f16)
    nb = scales.shape[1]
    small = jnp.concatenate([scales.astype(f16), hi, lo, jnp.zeros((own_rows, BLOCK - 2 - nb), f16)], 1)
    sent = jnp.concatenate([(quantized.astype(f32) * quant_up).astype(f16), small], 1)

    full = lax.all_gather(sent, ("tp", "sub"), axis=0, tiled=True)
    small_all = full[:, width:].astype(f32)
    full_quant = (full[:, :width].astype(f32) * (1.0 / quant_up)).astype(bf16)
    full_scales = small_all[:, :nb].astype(bf16)
    root_all = small_all[:, nb : nb + 1] + small_all[:, nb + 1 : nb + 2]
    me = d * sub + s
    q_own = lax.dynamic_slice_in_dim(full, me * BLOCK, BLOCK, 1).astype(f32) * (1.0 / quant_up)
    s_own = lax.dynamic_slice_in_dim(small_all, me, 1, 1)
    new_residual = (q_own * (s_own * root_all) / norm_gain.astype(f32)[None, :]).astype(bf16)
    return full_quant, full_scales, new_residual


def solution(mesh):
    in_specs = (
        P("rep", ("tp", "sub")),
        P(("tp", "sub"), None),
        P("rep", ("tp", "sub")),
        P(("tp", "sub")),
    )
    out_specs = (P("rep", None), P("rep", None), P("rep", ("tp", "sub")))
    return jax.shard_map(
        per_device, mesh=mesh, in_specs=in_specs, out_specs=out_specs, check_vma=False
    )
```

```python
import functools

import jax
import jax.numpy as jnp
from jax import lax
from jax.experimental import pallas as pl
from jax.experimental.pallas import tpu as pltpu
from jax.sharding import PartitionSpec as P

BLOCK = 128
epsilon = 0.1
floor_scale = 0.5
f32, f16, bf16 = jnp.float32, jnp.float16, jnp.bfloat16
sum_up = 4.0
quant_up = 2.0**14
STREAMS = 2
JUMP = 7


def arrange_kernel(chip_rows, order_ref, att_ref, res_ref, mine_ref, theirs_ref):
    n = mine_ref.shape[0] // chip_rows
    k = att_ref.shape[1]
    for out, base in ((mine_ref, 0), (theirs_ref, n)):
        for i in range(n):
            at = pl.multiple_of(order_ref[base + i], chip_rows)
            to = pl.ds(i * chip_rows, chip_rows)
            out[to, :k] = att_ref[pl.ds(at, chip_rows), :]
            out[to, k:] = res_ref[pl.ds(at, chip_rows), :]


def arrange(order, attention, residual, chip_rows):
    rows, k = attention.shape
    shape = jax.ShapeDtypeStruct((rows // 2, 2 * k), attention.dtype)
    return pl.pallas_call(
        functools.partial(arrange_kernel, chip_rows),
        in_specs=[pl.BlockSpec(memory_space=pltpu.SMEM)] + [pl.BlockSpec(memory_space=pltpu.VMEM)] * 2,
        out_specs=[pl.BlockSpec(memory_space=pltpu.VMEM)] * 2,
        out_shape=[shape, shape],
        compiler_params=pltpu.CompilerParams(vmem_limit_bytes=4 * 2**20),
    )(order, attention, residual)


def terms_kernel(chip_rows, first_step, steps, with_gain, place_ref, mine_ref, other_ref, gain_ref, w_ref, w_other_ref, *outs):
    k, cols = w_ref.shape
    chip_w = 2 * k
    d, s = place_ref[0], place_ref[1]
    step = pl.program_id(0)

    @pl.when(step < steps)
    def _():
        total = jnp.dot(mine_ref[:, :k], w_ref[...], preferred_element_type=f32)
        total += jnp.dot(other_ref[:, :k], w_other_ref[...], preferred_element_type=f32)
        total *= sum_up
        for i, out in enumerate(outs):
            out[...] = total[i * chip_rows : (i + 1) * chip_rows]

        per = cols // chip_w
        for j in range(per):
            @pl.when((first_step + step) * per + j == d)
            def _():
                a, b = mine_ref[:, k:].astype(f32) * sum_up, other_ref[:, k:].astype(f32) * sum_up
                first, second = jnp.where(s == 0, a, b), jnp.where(s == 0, b, a)
                for i, out in enumerate(outs):
                    at = slice(i * chip_rows, (i + 1) * chip_rows)
                    out[:, j * chip_w : j * chip_w + k] += first[at]
                    out[:, j * chip_w + k : (j + 1) * chip_w] += second[at]

    if with_gain:
        @pl.when(step == steps)
        def _():
            for out in outs:
                out[...] = gain_ref[...]


def terms(place, mine, other, gain, w, w_other, chip_rows, st, with_gain):
    width = w.shape[1] // STREAMS
    n = mine.shape[0] // chip_rows
    cols = gain.shape[1] * (1 if with_gain else 2)
    steps = width // cols
    extra = 1 if with_gain else 0
    whole = pl.BlockSpec(mine.shape, lambda i: (0, 0))
    weights = pl.BlockSpec((w.shape[0], cols), lambda i: (0, st * steps + jnp.minimum(i, steps - 1)))
    return pl.pallas_call(
        functools.partial(terms_kernel, chip_rows, st * steps, steps, with_gain),
        grid=(steps + extra,),
        in_specs=[
            pl.BlockSpec(memory_space=pltpu.SMEM), whole, whole,
            pl.BlockSpec(gain.shape, lambda i: (0, 0)), weights, weights,
        ],
        out_specs=[pl.BlockSpec((chip_rows, cols), lambda i: (0, i))] * n,
        out_shape=[jax.ShapeDtypeStruct((chip_rows, width + extra * cols), f32)] * n,
        compiler_params=pltpu.CompilerParams(vmem_limit_bytes=16 * 2**20),
        cost_estimate=pl.CostEstimate(
            flops=4 * mine.shape[0] * w.shape[0] * width, bytes_accessed=6 * 2**20, transcendentals=0
        ),
    )(place, mine, other, gain, w, w_other)


def per_device(attention, out_weight, residual, norm_gain):
    tp, sub = lax.axis_size("tp"), lax.axis_size("sub")
    d, s = lax.axis_index("tp"), lax.axis_index("sub")
    rows, width = attention.shape[0], out_weight.shape[1]
    chip_rows = rows // tp
    half = tp // 2
    swap = [(i, 1 - i) for i in range(sub)]
    up = [(sub * i, sub * ((i + 1) % tp)) for i in range(tp)]
    down = [(sub * i + 1, sub * ((i - 1) % tp) + 1) for i in range(tp)]

    slot = jnp.arange(half, dtype=jnp.int32)
    ahead = lax.rem(d + half - slot, tp)
    behind = jnp.where(slot == 0, d, lax.rem(d + half + slot, tp))
    order = jnp.where(s == 0, jnp.stack([ahead, behind]), jnp.stack([behind, ahead])) * chip_rows

    mine, theirs = arrange(order.reshape(-1), attention, residual, chip_rows)
    w_other = lax.ppermute(out_weight, "sub", swap)
    other = lax.ppermute(theirs, "sub", swap)
    gain_other = lax.ppermute(norm_gain, "sub", swap)
    gain_pair = jnp.where(s == 0, jnp.concatenate([norm_gain, gain_other]), jnp.concatenate([gain_other, norm_gain]))
    chip_w = gain_pair.shape[0]
    gain_w = width // chip_rows
    per_row = gain_w // chip_w
    pos_r = lax.broadcasted_iota(jnp.int32, (chip_rows, gain_w), 0)
    pos_c = lax.broadcasted_iota(jnp.int32, (chip_rows, gain_w), 1)
    at_own = pos_r * per_row + pos_c // chip_w == d
    gain_tile = jnp.where(at_own, jnp.tile(gain_pair, (per_row,)).astype(f32)[None, :], 0.0)

    me = (d * sub + s).astype(jnp.uint32)
    place, me, me_col = lax.optimization_barrier((jnp.stack([d, s]), me, me * BLOCK))
    zero = jnp.uint32(0)
    term = [
        terms(place, mine, other, gain_tile, out_weight, w_other, chip_rows, st, st == STREAMS - 1)
        for st in range(STREAMS)
    ]

    st_w = width // STREAMS
    far_up = [(sub * i, sub * ((i + JUMP) % tp)) for i in range(tp)]
    far_down = [(sub * i + 1, sub * ((i - JUMP) % tp) + 1) for i in range(tp)]
    pairs = [*up, *down]
    far_pairs = [*far_up, *far_down]

    class Chain:
        def __init__(self, st, first, last, links):
            self.st, self.at, self.last, self.links = st, first, last, links
            self.value = self.add(None)

        def add(self, got):
            own = term[self.st][self.at]
            return (own if got is None else got.astype(f32) + own).astype(f16)

        def step(self):
            done = self.at == self.last
            links = self.links if done else up if self.at == 0 else pairs
            got = lax.ppermute(self.value, ("tp", "sub"), links)
            if done:
                return got
            self.at += 1
            self.value = self.add(got)

    split = half - JUMP
    chains = [Chain(st, 0, split, far_pairs) for st in range(STREAMS)]
    chains += [Chain(st, split + 1, half - 1, pairs) for st in range(STREAMS)]
    ended = {}
    while len(ended) < len(chains):
        for i, chain in enumerate(chains):
            if i not in ended and (got := chain.step()) is not None:
                ended[i] = got.astype(f32)
    cur = []
    for st in range(STREAMS):
        both = ended[st] + ended[STREAMS + st]
        cur.append(jnp.where(s == 0, both, both + term[st][0]))
    cur_g = cur[-1][:, st_w:].astype(f16)
    cur[-1] = cur[-1][:, :st_w]
    whole = jnp.concatenate(cur, 1)
    own_rows = chip_rows // sub
    upper, lower = whole[:own_rows], whole[own_rows:]
    keep = jnp.where(s == 0, upper, lower)
    give = jnp.where(s == 0, lower, upper).astype(f16)
    hidden = (keep + lax.ppermute(give, "sub", swap).astype(f32)) * (1.0 / sum_up)
    gain_all = (cur_g.astype(f32) + lax.ppermute(cur_g, "sub", swap).astype(f32)).reshape(1, width)

    mean_square = jnp.sum(hidden * hidden, axis=1, keepdims=True) / width
    normed = hidden * lax.rsqrt(mean_square + epsilon) * gain_all
    blocks = normed.reshape(own_rows, width // BLOCK, BLOCK)
    scales = jnp.maximum(jnp.max(jnp.abs(blocks), axis=2), floor_scale).astype(bf16)
    quantized = (blocks / scales.astype(f32)[:, :, None]).reshape(own_rows, width).astype(bf16)
    root = jnp.sqrt(mean_square + epsilon)
    hi = root.astype(f16)
    lo = (root - hi.astype(f32)).astype(f16)
    nb = scales.shape[1]
    small = jnp.concatenate([scales.astype(f16), hi, lo, jnp.zeros((own_rows, BLOCK - 2 - nb), f16)], 1)
    sent = jnp.concatenate([(quantized.astype(f32) * quant_up).astype(f16), small], 1)

    full = lax.all_gather(sent, ("tp", "sub"), axis=0, tiled=True)
    small_all = full[:, width:].astype(f32)
    full_quant = (full[:, :width].astype(f32) * (1.0 / quant_up)).astype(bf16)
    full_scales = small_all[:, :nb].astype(bf16)
    root_all = small_all[:, nb : nb + 1] + small_all[:, nb + 1 : nb + 2]
    q_own = lax.dynamic_slice(full, (zero, me_col), (rows, BLOCK)).astype(f32) * (1.0 / quant_up)
    s_own = lax.dynamic_slice(small_all, (zero, me), (rows, 1))
    new_residual = (q_own * (s_own * root_all) / norm_gain.astype(f32)[None, :]).astype(bf16)
    return full_quant, full_scales, new_residual


def solution(mesh):
    in_specs = (
        P("rep", ("tp", "sub")),
        P(("tp", "sub"), None),
        P("rep", ("tp", "sub")),
        P(("tp", "sub")),
    )
    out_specs = (P("rep", None), P("rep", None), P("rep", ("tp", "sub")))
    return jax.shard_map(
        per_device, mesh=mesh, in_specs=in_specs, out_specs=out_specs, check_vma=False
    )
```

```python
import functools

import jax
import jax.numpy as jnp
from jax import lax
from jax.experimental import pallas as pl
from jax.experimental.pallas import tpu as pltpu
from jax.sharding import PartitionSpec as P

BLOCK = 128
epsilon = 0.1
floor_scale = 0.5
f32, f16, bf16 = jnp.float32, jnp.float16, jnp.bfloat16
sum_up = 4.0
quant_up = 2.0**14
STREAMS = 2
JUMP = 8


def arrange_kernel(chip_rows, order_ref, att_ref, res_ref, mine_ref, theirs_ref, att, res, sems):
    copies = [
        pltpu.make_async_copy(att_ref, att, sems.at[0]),
        pltpu.make_async_copy(res_ref, res, sems.at[1]),
    ]
    for copy in copies:
        copy.start()
    for copy in copies:
        copy.wait()
    n = mine_ref.shape[0] // chip_rows
    k = att.shape[1]
    for out, base in ((mine_ref, 0), (theirs_ref, n)):
        for i in range(n):
            at = pl.multiple_of(order_ref[base + i], chip_rows)
            to = pl.ds(i * chip_rows, chip_rows)
            out[to, :k] = att[pl.ds(at, chip_rows), :]
            out[to, k:] = res[pl.ds(at, chip_rows), :]


def arrange(order, attention, residual, chip_rows):
    rows, k = attention.shape
    shape = jax.ShapeDtypeStruct((rows // 2, 2 * k), attention.dtype)
    return pl.pallas_call(
        functools.partial(arrange_kernel, chip_rows),
        in_specs=[pl.BlockSpec(memory_space=pltpu.SMEM)] + [pl.BlockSpec(memory_space=pltpu.HBM)] * 2,
        out_specs=[pl.BlockSpec(memory_space=pltpu.VMEM)] * 2,
        out_shape=[shape, shape],
        scratch_shapes=[
            pltpu.VMEM(attention.shape, attention.dtype),
            pltpu.VMEM(residual.shape, residual.dtype),
            pltpu.SemaphoreType.DMA((2,)),
        ],
        compiler_params=pltpu.CompilerParams(vmem_limit_bytes=4 * 2**20),
    )(order, *[pltpu.with_memory_space_constraint(x, pltpu.HBM) for x in (attention, residual)])


def terms_kernel(chip_rows, first_step, steps, with_gain, place_ref, mine_ref, other_ref, gain_ref, w_ref, w_other_ref, *outs):
    k, cols = w_ref.shape
    chip_w = 2 * k
    d, s = place_ref[0], place_ref[1]
    step = pl.program_id(0)

    @pl.when(step < steps)
    def _():
        total = jnp.dot(mine_ref[:, :k], w_ref[...], preferred_element_type=f32)
        total += jnp.dot(other_ref[:, :k], w_other_ref[...], preferred_element_type=f32)
        total *= sum_up
        for i, out in enumerate(outs):
            out[...] = total[i * chip_rows : (i + 1) * chip_rows]

        per = cols // chip_w
        for j in range(per):
            @pl.when((first_step + step) * per + j == d)
            def _():
                a, b = mine_ref[:, k:].astype(f32) * sum_up, other_ref[:, k:].astype(f32) * sum_up
                first, second = jnp.where(s == 0, a, b), jnp.where(s == 0, b, a)
                for i, out in enumerate(outs):
                    at = slice(i * chip_rows, (i + 1) * chip_rows)
                    out[:, j * chip_w : j * chip_w + k] += first[at]
                    out[:, j * chip_w + k : (j + 1) * chip_w] += second[at]

    if with_gain:
        @pl.when(step == steps)
        def _():
            for out in outs:
                out[...] = gain_ref[...]


def terms(place, mine, other, gain, w, w_other, chip_rows, st, with_gain):
    width = w.shape[1] // STREAMS
    n = mine.shape[0] // chip_rows
    cols = gain.shape[1] * (1 if with_gain else 2)
    steps = width // cols
    extra = 1 if with_gain else 0
    whole = pl.BlockSpec(mine.shape, lambda i: (0, 0))
    weights = pl.BlockSpec((w.shape[0], cols), lambda i: (0, st * steps + jnp.minimum(i, steps - 1)))
    return pl.pallas_call(
        functools.partial(terms_kernel, chip_rows, st * steps, steps, with_gain),
        grid=(steps + extra,),
        in_specs=[
            pl.BlockSpec(memory_space=pltpu.SMEM), whole, whole,
            pl.BlockSpec(gain.shape, lambda i: (0, 0)), weights, weights,
        ],
        out_specs=[pl.BlockSpec((chip_rows, cols), lambda i: (0, i))] * n,
        out_shape=[jax.ShapeDtypeStruct((chip_rows, width + extra * cols), f32)] * n,
        compiler_params=pltpu.CompilerParams(vmem_limit_bytes=16 * 2**20),
        cost_estimate=pl.CostEstimate(
            flops=4 * mine.shape[0] * w.shape[0] * width, bytes_accessed=6 * 2**20, transcendentals=0
        ),
    )(place, mine, other, gain, w, w_other)


def per_device(attention, out_weight, residual, norm_gain):
    tp, sub = lax.axis_size("tp"), lax.axis_size("sub")
    d, s = lax.axis_index("tp"), lax.axis_index("sub")
    rows, width = attention.shape[0], out_weight.shape[1]
    chip_rows = rows // tp
    half = tp // 2
    swap = [(i, 1 - i) for i in range(sub)]
    up = [(sub * i, sub * ((i + 1) % tp)) for i in range(tp)]
    down = [(sub * i + 1, sub * ((i - 1) % tp) + 1) for i in range(tp)]

    slot = jnp.arange(half, dtype=jnp.int32)
    ahead = lax.rem(d + half - slot, tp)
    behind = jnp.where(slot == 0, d, lax.rem(d + half + slot, tp))
    order = jnp.where(s == 0, jnp.stack([ahead, behind]), jnp.stack([behind, ahead])) * chip_rows

    mine, theirs = arrange(order.reshape(-1), attention, residual, chip_rows)
    w_other = lax.ppermute(out_weight, "sub", swap)
    other = lax.ppermute(theirs, "sub", swap)
    gain_other = lax.ppermute(norm_gain, "sub", swap)
    gain_pair = jnp.where(s == 0, jnp.concatenate([norm_gain, gain_other]), jnp.concatenate([gain_other, norm_gain]))
    chip_w = gain_pair.shape[0]
    gain_w = width // chip_rows
    per_row = gain_w // chip_w
    pos_r = lax.broadcasted_iota(jnp.int32, (chip_rows, gain_w), 0)
    pos_c = lax.broadcasted_iota(jnp.int32, (chip_rows, gain_w), 1)
    at_own = pos_r * per_row + pos_c // chip_w == d
    gain_tile = jnp.where(at_own, jnp.tile(gain_pair, (per_row,)).astype(f32)[None, :], 0.0)

    me = (d * sub + s).astype(jnp.uint32)
    place, me, me_col = lax.optimization_barrier((jnp.stack([d, s]), me, me * BLOCK))
    zero = jnp.uint32(0)
    w_own = pltpu.with_memory_space_constraint(out_weight, pltpu.HBM)
    term = [
        terms(place, mine, other, gain_tile, w_own, w_other, chip_rows, st, st == STREAMS - 1)
        for st in range(STREAMS)
    ]

    st_w = width // STREAMS
    far_up = [(sub * i, sub * ((i + JUMP) % tp)) for i in range(tp)]
    far_down = [(sub * i + 1, sub * ((i - JUMP) % tp) + 1) for i in range(tp)]
    pairs = [*up, *down]
    far_pairs = [*far_up, *far_down]

    class Chain:
        def __init__(self, st, first, last, links):
            self.st, self.at, self.last, self.links = st, first, last, links
            self.value = self.add(None)
            if first == 0:
                self.value = jnp.where(s == 0, self.value, jnp.zeros_like(self.value))

        def add(self, got):
            own = term[self.st][self.at]
            return (own if got is None else got.astype(f32) + own).astype(f16)

        def step(self):
            done = self.at == self.last
            links = self.links if done else pairs
            got = lax.ppermute(self.value, ("tp", "sub"), links)
            if done:
                return got
            self.at += 1
            self.value = self.add(got)

    split = half - JUMP
    chains = [Chain(st, 0, split, far_pairs) for st in range(STREAMS)]
    chains += [Chain(st, split + 1, half - 1, pairs) for st in range(STREAMS)]
    ended = {}
    while len(ended) < len(chains):
        for i, chain in enumerate(chains):
            if i not in ended and (got := chain.step()) is not None:
                ended[i] = got.astype(f32)
    cur = []
    for st in range(STREAMS):
        both = ended[st] + ended[STREAMS + st]
        cur.append(jnp.where(s == 0, both, both + term[st][0]))
    cur_g = cur[-1][:, st_w:].astype(f16)
    cur[-1] = cur[-1][:, :st_w]
    whole = jnp.concatenate(cur, 1)
    own_rows = chip_rows // sub
    upper, lower = whole[:own_rows], whole[own_rows:]
    keep = jnp.where(s == 0, upper, lower)
    give = jnp.where(s == 0, lower, upper).astype(f16)
    hidden = (keep + lax.ppermute(give, "sub", swap).astype(f32)) * (1.0 / sum_up)
    gain_all = (cur_g.astype(f32) + lax.ppermute(cur_g, "sub", swap).astype(f32)).reshape(1, width)

    mean_square = jnp.sum(hidden * hidden, axis=1, keepdims=True) / width
    normed = hidden * lax.rsqrt(mean_square + epsilon) * gain_all
    blocks = normed.reshape(own_rows, width // BLOCK, BLOCK)
    scales = jnp.maximum(jnp.max(jnp.abs(blocks), axis=2), floor_scale).astype(bf16)
    quantized = (blocks / scales.astype(f32)[:, :, None]).reshape(own_rows, width).astype(bf16)
    root = jnp.sqrt(mean_square + epsilon)
    hi = root.astype(f16)
    lo = (root - hi.astype(f32)).astype(f16)
    nb = scales.shape[1]
    small = jnp.concatenate([scales.astype(f16), hi, lo, jnp.zeros((own_rows, BLOCK - 2 - nb), f16)], 1)
    sent = jnp.concatenate([(quantized.astype(f32) * quant_up).astype(f16), small], 1)

    full = lax.all_gather(sent, ("tp", "sub"), axis=0, tiled=True)
    small_all = full[:, width:].astype(f32)
    full_quant = (full[:, :width].astype(f32) * (1.0 / quant_up)).astype(bf16)
    full_scales = small_all[:, :nb].astype(bf16)
    root_all = small_all[:, nb : nb + 1] + small_all[:, nb + 1 : nb + 2]
    q_own = lax.dynamic_slice(full, (zero, me_col), (rows, BLOCK)).astype(f32) * (1.0 / quant_up)
    s_own = lax.dynamic_slice(small_all, (zero, me), (rows, 1))
    new_residual = (q_own * (s_own * root_all) / norm_gain.astype(f32)[None, :]).astype(bf16)
    return full_quant, full_scales, new_residual


def solution(mesh):
    in_specs = (
        P("rep", ("tp", "sub")),
        P(("tp", "sub"), None),
        P("rep", ("tp", "sub")),
        P(("tp", "sub")),
    )
    out_specs = (P("rep", None), P("rep", None), P("rep", ("tp", "sub")))
    return jax.shard_map(
        per_device, mesh=mesh, in_specs=in_specs, out_specs=out_specs, check_vma=False
    )
```

```python
import functools

import jax
import jax.numpy as jnp
from jax import lax
from jax.experimental import pallas as pl
from jax.experimental.pallas import tpu as pltpu
from jax.sharding import PartitionSpec as P

BLOCK = 128
epsilon = 0.1
floor_scale = 0.5
f32, f16, bf16 = jnp.float32, jnp.float16, jnp.bfloat16
sum_up = 4.0
quant_up = 2.0**14
STREAMS = 2
JUMP = 9


def arrange_kernel(chip_rows, order_ref, att_ref, res_ref, mine_ref, theirs_ref, att, res, sems):
    copies = [
        pltpu.make_async_copy(att_ref, att, sems.at[0]),
        pltpu.make_async_copy(res_ref, res, sems.at[1]),
    ]
    for copy in copies:
        copy.start()
    for copy in copies:
        copy.wait()
    n = mine_ref.shape[0] // chip_rows
    k = att.shape[1]
    for out, base in ((mine_ref, 0), (theirs_ref, n)):
        for i in range(n):
            at = pl.multiple_of(order_ref[base + i], chip_rows)
            to = pl.ds(i * chip_rows, chip_rows)
            out[to, :k] = att[pl.ds(at, chip_rows), :]
            out[to, k:] = res[pl.ds(at, chip_rows), :]


def arrange(order, attention, residual, chip_rows):
    rows, k = attention.shape
    shape = jax.ShapeDtypeStruct((rows // 2, 2 * k), attention.dtype)
    return pl.pallas_call(
        functools.partial(arrange_kernel, chip_rows),
        in_specs=[pl.BlockSpec(memory_space=pltpu.SMEM)] + [pl.BlockSpec(memory_space=pltpu.HBM)] * 2,
        out_specs=[pl.BlockSpec(memory_space=pltpu.VMEM)] * 2,
        out_shape=[shape, shape],
        scratch_shapes=[
            pltpu.VMEM(attention.shape, attention.dtype),
            pltpu.VMEM(residual.shape, residual.dtype),
            pltpu.SemaphoreType.DMA((2,)),
        ],
        compiler_params=pltpu.CompilerParams(vmem_limit_bytes=4 * 2**20),
    )(order, *[pltpu.with_memory_space_constraint(x, pltpu.HBM) for x in (attention, residual)])


def terms_kernel(chip_rows, first_step, steps, with_gain, place_ref, mine_ref, other_ref, w_ref, w_other_ref, *rest):
    gain_ref, outs = (rest[0], rest[1:]) if with_gain else (None, rest)
    k, cols = w_ref.shape
    chip_w = 2 * k
    d, s = place_ref[0], place_ref[1]
    step = pl.program_id(0)

    @pl.when(step < steps)
    def _():
        left = jnp.concatenate([mine_ref[:, :k], other_ref[:, :k]], 1)
        right = jnp.concatenate([w_ref[...], w_other_ref[...]], 0)
        total = jnp.dot(left, right, preferred_element_type=f32) * sum_up
        for i, out in enumerate(outs):
            out[...] = total[i * chip_rows : (i + 1) * chip_rows]

        per = cols // chip_w
        for j in range(per):
            @pl.when((first_step + step) * per + j == d)
            def _():
                a, b = mine_ref[:, k:].astype(f32) * sum_up, other_ref[:, k:].astype(f32) * sum_up
                first, second = jnp.where(s == 0, a, b), jnp.where(s == 0, b, a)
                for i, out in enumerate(outs):
                    at = slice(i * chip_rows, (i + 1) * chip_rows)
                    out[:, j * chip_w : j * chip_w + k] += first[at]
                    out[:, j * chip_w + k : (j + 1) * chip_w] += second[at]

    if with_gain:
        @pl.when(step == steps)
        def _():
            for out in outs:
                out[...] = gain_ref[...]


def terms(place, mine, other, gain, w, w_other, chip_rows, st, with_gain):
    width = w.shape[1] // STREAMS
    n = mine.shape[0] // chip_rows
    cols = gain.shape[1] * (1 if with_gain else 2)
    steps = width // cols
    extra = 1 if with_gain else 0
    whole = pl.BlockSpec(mine.shape, lambda i: (0, 0))
    weights = pl.BlockSpec((w.shape[0], cols), lambda i: (0, st * steps + jnp.minimum(i, steps - 1)))
    return pl.pallas_call(
        functools.partial(terms_kernel, chip_rows, st * steps, steps, with_gain),
        grid=(steps + extra,),
        in_specs=[
            pl.BlockSpec(memory_space=pltpu.SMEM), whole, whole, weights, weights,
            *[pl.BlockSpec(gain.shape, lambda i: (0, 0))] * extra,
        ],
        out_specs=[pl.BlockSpec((chip_rows, cols), lambda i: (0, i))] * n,
        out_shape=[jax.ShapeDtypeStruct((chip_rows, width + extra * cols), f32)] * n,
        compiler_params=pltpu.CompilerParams(vmem_limit_bytes=16 * 2**20),
        cost_estimate=pl.CostEstimate(
            flops=4 * mine.shape[0] * w.shape[0] * width, bytes_accessed=6 * 2**20, transcendentals=0
        ),
    )(place, mine, other, w, w_other, *[gain] * extra)


def per_device(attention, out_weight, residual, norm_gain):
    tp, sub = lax.axis_size("tp"), lax.axis_size("sub")
    d, s = lax.axis_index("tp"), lax.axis_index("sub")
    rows, width = attention.shape[0], out_weight.shape[1]
    chip_rows = rows // tp
    half = tp // 2
    swap = [(i, 1 - i) for i in range(sub)]
    up = [(sub * i, sub * ((i + 1) % tp)) for i in range(tp)]
    down = [(sub * i + 1, sub * ((i - 1) % tp) + 1) for i in range(tp)]

    slot = jnp.arange(half, dtype=jnp.int32)
    ahead = lax.rem(d + half - slot, tp)
    behind = jnp.where(slot == 0, d, lax.rem(d + half + slot, tp))
    order = jnp.where(s == 0, jnp.stack([ahead, behind]), jnp.stack([behind, ahead])) * chip_rows

    mine, theirs = arrange(order.reshape(-1), attention, residual, chip_rows)
    w_other = lax.ppermute(out_weight, "sub", swap)
    other = lax.ppermute(theirs, "sub", swap)
    gain_other = lax.ppermute(norm_gain, "sub", swap)
    gain_pair = jnp.where(s == 0, jnp.concatenate([norm_gain, gain_other]), jnp.concatenate([gain_other, norm_gain]))
    chip_w = gain_pair.shape[0]
    gain_w = width // chip_rows
    per_row = gain_w // chip_w
    pos_r = lax.broadcasted_iota(jnp.int32, (chip_rows, gain_w), 0)
    pos_c = lax.broadcasted_iota(jnp.int32, (chip_rows, gain_w), 1)
    at_own = pos_r * per_row + pos_c // chip_w == d
    gain_tile = jnp.where(at_own, jnp.tile(gain_pair, (per_row,)).astype(f32)[None, :], 0.0)

    me = (d * sub + s).astype(jnp.uint32)
    place, me, me_col = lax.optimization_barrier((jnp.stack([d, s]), me, me * BLOCK))
    zero = jnp.uint32(0)
    w_own = pltpu.with_memory_space_constraint(out_weight, pltpu.HBM)
    term = [
        terms(place, mine, other, gain_tile, w_own, w_other, chip_rows, st, st == STREAMS - 1)
        for st in range(STREAMS)
    ]

    st_w = width // STREAMS
    far_up = [(sub * i, sub * ((i + JUMP) % tp)) for i in range(tp)]
    far_down = [(sub * i + 1, sub * ((i - JUMP) % tp) + 1) for i in range(tp)]
    pairs = [*up, *down]
    far_pairs = [*far_up, *far_down]

    class Chain:
        def __init__(self, st, first, last, links):
            self.st, self.at, self.last, self.links = st, first, last, links
            self.value = self.add(None)
            if first == 0:
                self.value = jnp.where(s == 0, self.value, jnp.zeros_like(self.value))

        def add(self, got):
            own = term[self.st][self.at]
            return (own if got is None else got.astype(f32) + own).astype(f16)

        def step(self):
            done = self.at == self.last
            links = self.links if done else pairs
            got = lax.ppermute(self.value, ("tp", "sub"), links)
            if done:
                return got
            self.at += 1
            self.value = self.add(got)

    split = half - JUMP
    chains = [Chain(st, 0, split, far_pairs) for st in range(STREAMS)]
    chains += [Chain(st, split + 1, half - 1, pairs) for st in range(STREAMS)]
    ended = {}
    while len(ended) < len(chains):
        for i, chain in enumerate(chains):
            if i not in ended and (got := chain.step()) is not None:
                ended[i] = got.astype(f32)
    cur = []
    for st in range(STREAMS):
        both = ended[st] + ended[STREAMS + st]
        cur.append(jnp.where(s == 0, both, both + term[st][0]))
    cur_g = cur[-1][:, st_w:].astype(f16)
    cur[-1] = cur[-1][:, :st_w]
    whole = jnp.concatenate(cur, 1)
    own_rows = chip_rows // sub
    upper, lower = whole[:own_rows], whole[own_rows:]
    keep = jnp.where(s == 0, upper, lower)
    give = jnp.where(s == 0, lower, upper).astype(f16)
    hidden = (keep + lax.ppermute(give, "sub", swap).astype(f32)) * (1.0 / sum_up)
    gain_all = (cur_g.astype(f32) + lax.ppermute(cur_g, "sub", swap).astype(f32)).reshape(1, width)

    mean_square = jnp.sum(hidden * hidden, axis=1, keepdims=True) / width
    normed = hidden * lax.rsqrt(mean_square + epsilon) * gain_all
    blocks = normed.reshape(own_rows, width // BLOCK, BLOCK)
    scales = jnp.maximum(jnp.max(jnp.abs(blocks), axis=2), floor_scale).astype(bf16)
    quantized = (blocks / scales.astype(f32)[:, :, None]).reshape(own_rows, width).astype(bf16)
    root = jnp.sqrt(mean_square + epsilon)
    hi = root.astype(f16)
    lo = (root - hi.astype(f32)).astype(f16)
    nb = scales.shape[1]
    small = jnp.concatenate([scales.astype(f16), hi, lo, jnp.zeros((own_rows, BLOCK - 2 - nb), f16)], 1)
    sent = jnp.concatenate([(quantized.astype(f32) * quant_up).astype(f16), small], 1)

    full = lax.all_gather(sent, ("tp", "sub"), axis=0, tiled=True)
    small_all = full[:, width:].astype(f32)
    full_quant = (full[:, :width].astype(f32) * (1.0 / quant_up)).astype(bf16)
    full_scales = small_all[:, :nb].astype(bf16)
    root_all = small_all[:, nb : nb + 1] + small_all[:, nb + 1 : nb + 2]
    q_own = lax.dynamic_slice(full, (zero, me_col), (rows, BLOCK)).astype(f32) * (1.0 / quant_up)
    s_own = lax.dynamic_slice(small_all, (zero, me), (rows, 1))
    new_residual = (q_own * (s_own * root_all) / norm_gain.astype(f32)[None, :]).astype(bf16)
    return full_quant, full_scales, new_residual


def solution(mesh):
    in_specs = (
        P("rep", ("tp", "sub")),
        P(("tp", "sub"), None),
        P("rep", ("tp", "sub")),
        P(("tp", "sub")),
    )
    out_specs = (P("rep", None), P("rep", None), P("rep", ("tp", "sub")))
    return jax.shard_map(
        per_device, mesh=mesh, in_specs=in_specs, out_specs=out_specs, check_vma=False
    )
```

```python
import functools

import jax
import jax.numpy as jnp
from jax import lax
from jax.experimental import pallas as pl
from jax.experimental.pallas import tpu as pltpu
from jax.sharding import PartitionSpec as P

BLOCK = 128
epsilon = 0.1
floor_scale = 0.5
f32, f16, bf16 = jnp.float32, jnp.float16, jnp.bfloat16
sum_up = 4.0
quant_up = 2.0**14
STREAMS = 2
JUMP = 10


def arrange_kernel(chip_rows, order_ref, att_ref, res_ref, mine_ref, theirs_ref, att, res, sems):
    copies = [
        pltpu.make_async_copy(att_ref, att, sems.at[0]),
        pltpu.make_async_copy(res_ref, res, sems.at[1]),
    ]
    for copy in copies:
        copy.start()
    for copy in copies:
        copy.wait()
    n = mine_ref.shape[0] // chip_rows
    k = att.shape[1]
    for out, base in ((mine_ref, 0), (theirs_ref, n)):
        for i in range(n):
            at = pl.multiple_of(order_ref[base + i], chip_rows)
            to = pl.ds(i * chip_rows, chip_rows)
            out[to, :k] = att[pl.ds(at, chip_rows), :]
            out[to, k:] = res[pl.ds(at, chip_rows), :]


def arrange(order, attention, residual, chip_rows):
    rows, k = attention.shape
    shape = jax.ShapeDtypeStruct((rows // 2, 2 * k), attention.dtype)
    return pl.pallas_call(
        functools.partial(arrange_kernel, chip_rows),
        in_specs=[pl.BlockSpec(memory_space=pltpu.SMEM)] + [pl.BlockSpec(memory_space=pltpu.HBM)] * 2,
        out_specs=[pl.BlockSpec(memory_space=pltpu.VMEM)] * 2,
        out_shape=[shape, shape],
        scratch_shapes=[
            pltpu.VMEM(attention.shape, attention.dtype),
            pltpu.VMEM(residual.shape, residual.dtype),
            pltpu.SemaphoreType.DMA((2,)),
        ],
        compiler_params=pltpu.CompilerParams(vmem_limit_bytes=4 * 2**20),
    )(order, *[pltpu.with_memory_space_constraint(x, pltpu.HBM) for x in (attention, residual)])


COLS = 1024


def terms_kernel(chip_rows, first_step, steps, with_gain, place_ref, mine_ref, other_ref, w_ref, w_other_ref, *rest):
    gain_ref, outs = (rest[0], rest[1:]) if with_gain else (None, rest)
    k, cols = w_ref.shape
    chip_w = 2 * k
    d, s = place_ref[0], place_ref[1]
    step = pl.program_id(0)

    @pl.when(step < steps)
    def _():
        left = jnp.concatenate([mine_ref[:, :k], other_ref[:, :k]], 1)
        right = jnp.concatenate([w_ref[...], w_other_ref[...]], 0)
        total = jnp.dot(left, right, preferred_element_type=f32) * sum_up
        for i, out in enumerate(outs):
            out[...] = total[i * chip_rows : (i + 1) * chip_rows]

        per = cols // chip_w
        for j in range(per):
            @pl.when((first_step + step) * per + j == d)
            def _():
                a, b = mine_ref[:, k:].astype(f32) * sum_up, other_ref[:, k:].astype(f32) * sum_up
                first, second = jnp.where(s == 0, a, b), jnp.where(s == 0, b, a)
                for i, out in enumerate(outs):
                    at = slice(i * chip_rows, (i + 1) * chip_rows)
                    out[:, j * chip_w : j * chip_w + k] += first[at]
                    out[:, j * chip_w + k : (j + 1) * chip_w] += second[at]

    if with_gain:
        @pl.when(step == steps)
        def _():
            for out in outs:
                out[...] = gain_ref[...]


def terms(place, mine, other, gain, w, w_other, chip_rows, st, with_gain):
    width = w.shape[1] // STREAMS
    n = mine.shape[0] // chip_rows
    cols = gain.shape[1] if with_gain else COLS
    steps = width // cols
    extra = 1 if with_gain else 0
    whole = pl.BlockSpec(mine.shape, lambda i: (0, 0))
    weights = pl.BlockSpec((w.shape[0], cols), lambda i: (0, st * steps + jnp.minimum(i, steps - 1)))
    return pl.pallas_call(
        functools.partial(terms_kernel, chip_rows, st * steps, steps, with_gain),
        grid=(steps + extra,),
        in_specs=[
            pl.BlockSpec(memory_space=pltpu.SMEM), whole, whole, weights, weights,
            *[pl.BlockSpec(gain.shape, lambda i: (0, 0)) for _ in range(extra)],
        ],
        out_specs=[pl.BlockSpec((chip_rows, cols), lambda i: (0, i))] * n,
        out_shape=[jax.ShapeDtypeStruct((chip_rows, width + extra * cols), f32)] * n,
        compiler_params=pltpu.CompilerParams(vmem_limit_bytes=16 * 2**20),
        cost_estimate=pl.CostEstimate(
            flops=4 * mine.shape[0] * w.shape[0] * width, bytes_accessed=6 * 2**20, transcendentals=0
        ),
    )(place, mine, other, w, w_other, *[gain] * extra)


def per_device(attention, out_weight, residual, norm_gain):
    tp, sub = lax.axis_size("tp"), lax.axis_size("sub")
    d, s = lax.axis_index("tp"), lax.axis_index("sub")
    rows, width = attention.shape[0], out_weight.shape[1]
    chip_rows = rows // tp
    half = tp // 2
    swap = [(i, 1 - i) for i in range(sub)]
    up = [(sub * i, sub * ((i + 1) % tp)) for i in range(tp)]
    down = [(sub * i + 1, sub * ((i - 1) % tp) + 1) for i in range(tp)]

    slot = jnp.arange(half, dtype=jnp.int32)
    ahead = lax.rem(d + half - slot, tp)
    behind = jnp.where(slot == 0, d, lax.rem(d + half + slot, tp))
    order = jnp.where(s == 0, jnp.stack([ahead, behind]), jnp.stack([behind, ahead])) * chip_rows

    mine, theirs = arrange(order.reshape(-1), attention, residual, chip_rows)
    w_other = lax.ppermute(out_weight, "sub", swap)
    other = lax.ppermute(theirs, "sub", swap)
    gain_other = lax.ppermute(norm_gain, "sub", swap)
    me = (d * sub + s).astype(jnp.uint32)
    place, me, me_col = lax.optimization_barrier((jnp.stack([d, s]), me, me * BLOCK))
    zero = jnp.uint32(0)
    w_own = pltpu.with_memory_space_constraint(out_weight, pltpu.HBM)
    term = [list(terms(place, mine, other, None, w_own, w_other, chip_rows, st, False)) for st in range(STREAMS - 1)]
    term[0][0], gain_other = lax.optimization_barrier((term[0][0], gain_other))
    gain_pair = jnp.where(s == 0, jnp.concatenate([norm_gain, gain_other]), jnp.concatenate([gain_other, norm_gain]))
    chip_w = gain_pair.shape[0]
    gain_w = width // chip_rows
    per_row = gain_w // chip_w
    pos_r = lax.broadcasted_iota(jnp.int32, (chip_rows, gain_w), 0)
    pos_c = lax.broadcasted_iota(jnp.int32, (chip_rows, gain_w), 1)
    at_own = pos_r * per_row + pos_c // chip_w == d
    gain_tile = jnp.where(at_own, jnp.tile(gain_pair, (per_row,)).astype(f32)[None, :], 0.0)

    term.append(terms(place, mine, other, gain_tile, w_own, w_other, chip_rows, STREAMS - 1, True))

    st_w = width // STREAMS
    far_up = [(sub * i, sub * ((i + JUMP) % tp)) for i in range(tp)]
    far_down = [(sub * i + 1, sub * ((i - JUMP) % tp) + 1) for i in range(tp)]
    pairs = [*up, *down]
    far_pairs = [*far_up, *far_down]

    class Chain:
        def __init__(self, st, first, last, links):
            self.st, self.at, self.last, self.links = st, first, last, links
            self.value = self.add(None)
            if first == 0:
                self.value = jnp.where(s == 0, self.value, jnp.zeros_like(self.value))

        def add(self, got):
            own = term[self.st][self.at]
            return (own if got is None else got.astype(f32) + own).astype(f16)

        def step(self):
            done = self.at == self.last
            links = self.links if done else pairs
            got = lax.ppermute(self.value, ("tp", "sub"), links)
            if done:
                return got
            self.at += 1
            self.value = self.add(got)

    split = half - JUMP
    chains = [Chain(st, 0, split, far_pairs) for st in range(STREAMS)]
    chains += [Chain(st, split + 1, half - 1, pairs) for st in range(STREAMS)]
    ended = {}
    while len(ended) < len(chains):
        for i, chain in enumerate(chains):
            if i not in ended and (got := chain.step()) is not None:
                ended[i] = got.astype(f32)
    cur = []
    for st in range(STREAMS):
        both = ended[st] + ended[STREAMS + st]
        cur.append(jnp.where(s == 0, both, both + term[st][0]))
    cur_g = cur[-1][:, st_w:].astype(f16)
    cur[-1] = cur[-1][:, :st_w]
    whole = jnp.concatenate(cur, 1)
    own_rows = chip_rows // sub
    upper, lower = whole[:own_rows], whole[own_rows:]
    keep = jnp.where(s == 0, upper, lower)
    give = jnp.where(s == 0, lower, upper).astype(f16)
    hidden = (keep + lax.ppermute(give, "sub", swap).astype(f32)) * (1.0 / sum_up)
    gain_all = (cur_g.astype(f32) + lax.ppermute(cur_g, "sub", swap).astype(f32)).reshape(1, width)

    mean_square = jnp.sum(hidden * hidden, axis=1, keepdims=True) / width
    normed = hidden * lax.rsqrt(mean_square + epsilon) * gain_all
    blocks = normed.reshape(own_rows, width // BLOCK, BLOCK)
    scales = jnp.maximum(jnp.max(jnp.abs(blocks), axis=2), floor_scale).astype(bf16)
    quantized = (blocks / scales.astype(f32)[:, :, None]).reshape(own_rows, width).astype(bf16)
    root = jnp.sqrt(mean_square + epsilon)
    hi = root.astype(f16)
    lo = (root - hi.astype(f32)).astype(f16)
    nb = scales.shape[1]
    small = jnp.concatenate([scales.astype(f16), hi, lo, jnp.zeros((own_rows, BLOCK - 2 - nb), f16)], 1)
    sent = jnp.concatenate([(quantized.astype(f32) * quant_up).astype(f16), small], 1)

    full = lax.all_gather(sent, ("tp", "sub"), axis=0, tiled=True)
    small_all = full[:, width:].astype(f32)
    full_quant = (full[:, :width].astype(f32) * (1.0 / quant_up)).astype(bf16)
    full_scales = small_all[:, :nb].astype(bf16)
    root_all = small_all[:, nb : nb + 1] + small_all[:, nb + 1 : nb + 2]
    q_own = lax.dynamic_slice(full, (zero, me_col), (rows, BLOCK)).astype(f32) * (1.0 / quant_up)
    s_own = lax.dynamic_slice(small_all, (zero, me), (rows, 1))
    new_residual = (q_own * (s_own * root_all) / norm_gain.astype(f32)[None, :]).astype(bf16)
    return full_quant, full_scales, new_residual


def solution(mesh):
    in_specs = (
        P("rep", ("tp", "sub")),
        P(("tp", "sub"), None),
        P("rep", ("tp", "sub")),
        P(("tp", "sub")),
    )
    out_specs = (P("rep", None), P("rep", None), P("rep", ("tp", "sub")))
    return jax.shard_map(
        per_device, mesh=mesh, in_specs=in_specs, out_specs=out_specs, check_vma=False
    )
```

```python
import functools

import jax
import jax.numpy as jnp
from jax import lax
from jax.experimental import pallas as pl
from jax.experimental.pallas import tpu as pltpu
from jax.sharding import PartitionSpec as P

BLOCK = 128
epsilon = 0.1
floor_scale = 0.5
f32, f16, bf16 = jnp.float32, jnp.float16, jnp.bfloat16
sum_up = 4.0
quant_up = 2.0**14
STREAMS = 2
JUMP = 9


def arrange_kernel(chip_rows, order_ref, att_ref, res_ref, mine_ref, theirs_ref, att, res, sems):
    copies = [
        pltpu.make_async_copy(att_ref, att, sems.at[0]),
        pltpu.make_async_copy(res_ref, res, sems.at[1]),
    ]
    for copy in copies:
        copy.start()
    for copy in copies:
        copy.wait()
    n = mine_ref.shape[0] // chip_rows
    k = att.shape[1]
    for out, base in ((mine_ref, 0), (theirs_ref, n)):
        for i in range(n):
            at = pl.multiple_of(order_ref[base + i], chip_rows)
            to = pl.ds(i * chip_rows, chip_rows)
            out[to, :k] = att[pl.ds(at, chip_rows), :]
            out[to, k:] = res[pl.ds(at, chip_rows), :]


def arrange(order, attention, residual, chip_rows):
    rows, k = attention.shape
    shape = jax.ShapeDtypeStruct((rows // 2, 2 * k), attention.dtype)
    return pl.pallas_call(
        functools.partial(arrange_kernel, chip_rows),
        in_specs=[pl.BlockSpec(memory_space=pltpu.SMEM)] + [pl.BlockSpec(memory_space=pltpu.HBM)] * 2,
        out_specs=[pl.BlockSpec(memory_space=pltpu.VMEM)] * 2,
        out_shape=[shape, shape],
        scratch_shapes=[
            pltpu.VMEM(attention.shape, attention.dtype),
            pltpu.VMEM(residual.shape, residual.dtype),
            pltpu.SemaphoreType.DMA((2,)),
        ],
        compiler_params=pltpu.CompilerParams(vmem_limit_bytes=4 * 2**20),
    )(order, *[pltpu.with_memory_space_constraint(x, pltpu.HBM) for x in (attention, residual)])


COLS = 1024


def terms_kernel(chip_rows, first_step, steps, with_gain, place_ref, mine_ref, other_ref, w_ref, w_other_ref, *rest):
    gain_ref, outs = (rest[0], rest[1:]) if with_gain else (None, rest)
    k, cols = w_ref.shape
    chip_w = 2 * k
    d, s = place_ref[0], place_ref[1]
    step = pl.program_id(0)

    @pl.when(step < steps)
    def _():
        left = jnp.concatenate([mine_ref[:, :k], other_ref[:, :k]], 1)
        right = jnp.concatenate([w_ref[...], w_other_ref[...]], 0)
        total = jnp.dot(left, right, preferred_element_type=f32) * sum_up
        for i, out in enumerate(outs):
            out[...] = total[i * chip_rows : (i + 1) * chip_rows]

        per = cols // chip_w
        for j in range(per):
            @pl.when((first_step + step) * per + j == d)
            def _():
                a, b = mine_ref[:, k:].astype(f32) * sum_up, other_ref[:, k:].astype(f32) * sum_up
                first, second = jnp.where(s == 0, a, b), jnp.where(s == 0, b, a)
                for i, out in enumerate(outs):
                    at = slice(i * chip_rows, (i + 1) * chip_rows)
                    out[:, j * chip_w : j * chip_w + k] += first[at]
                    out[:, j * chip_w + k : (j + 1) * chip_w] += second[at]

    if with_gain:
        @pl.when(step == steps)
        def _():
            for out in outs:
                out[...] = gain_ref[...]


def terms(place, mine, other, gain, w, w_other, chip_rows, st, with_gain):
    width = w.shape[1] // STREAMS
    n = mine.shape[0] // chip_rows
    cols = gain.shape[1] if with_gain else COLS
    steps = width // cols
    extra = 1 if with_gain else 0
    whole = pl.BlockSpec(mine.shape, lambda i: (0, 0))
    weights = pl.BlockSpec((w.shape[0], cols), lambda i: (0, st * steps + jnp.minimum(i, steps - 1)))
    return pl.pallas_call(
        functools.partial(terms_kernel, chip_rows, st * steps, steps, with_gain),
        grid=(steps + extra,),
        in_specs=[
            pl.BlockSpec(memory_space=pltpu.SMEM), whole, whole, weights, weights,
            *[pl.BlockSpec(gain.shape, lambda i: (0, 0)) for _ in range(extra)],
        ],
        out_specs=[pl.BlockSpec((chip_rows, cols), lambda i: (0, i))] * n,
        out_shape=[jax.ShapeDtypeStruct((chip_rows, width + extra * cols), f32)] * n,
        compiler_params=pltpu.CompilerParams(vmem_limit_bytes=16 * 2**20),
        cost_estimate=pl.CostEstimate(
            flops=4 * mine.shape[0] * w.shape[0] * width, bytes_accessed=6 * 2**20, transcendentals=0
        ),
    )(place, mine, other, w, w_other, *[gain] * extra)


def per_device(attention, out_weight, residual, norm_gain):
    tp, sub = lax.axis_size("tp"), lax.axis_size("sub")
    d, s = lax.axis_index("tp"), lax.axis_index("sub")
    rows, width = attention.shape[0], out_weight.shape[1]
    chip_rows = rows // tp
    half = tp // 2
    swap = [(i, 1 - i) for i in range(sub)]
    up = [(sub * i, sub * ((i + 1) % tp)) for i in range(tp)]
    down = [(sub * i + 1, sub * ((i - 1) % tp) + 1) for i in range(tp)]

    slot = jnp.arange(half, dtype=jnp.int32)
    ahead = lax.rem(d + half - slot, tp)
    behind = jnp.where(slot == 0, d, lax.rem(d + half + slot, tp))
    order = jnp.where(s == 0, jnp.stack([ahead, behind]), jnp.stack([behind, ahead])) * chip_rows

    mine, theirs = arrange(order.reshape(-1), attention, residual, chip_rows)
    w_other = lax.ppermute(out_weight, "sub", swap)
    other = lax.ppermute(theirs, "sub", swap)
    gain_other = lax.ppermute(norm_gain, "sub", swap)
    me = (d * sub + s).astype(jnp.uint32)
    place, me, me_col = lax.optimization_barrier((jnp.stack([d, s]), me, me * BLOCK))
    zero = jnp.uint32(0)
    w_own = pltpu.with_memory_space_constraint(out_weight, pltpu.HBM)
    term = [list(terms(place, mine, other, None, w_own, w_other, chip_rows, st, False)) for st in range(STREAMS - 1)]
    term[0][0], gain_other = lax.optimization_barrier((term[0][0], gain_other))
    gain_pair = jnp.where(s == 0, jnp.concatenate([norm_gain, gain_other]), jnp.concatenate([gain_other, norm_gain]))
    chip_w = gain_pair.shape[0]
    gain_w = width // chip_rows
    per_row = gain_w // chip_w
    pos_r = lax.broadcasted_iota(jnp.int32, (chip_rows, gain_w), 0)
    pos_c = lax.broadcasted_iota(jnp.int32, (chip_rows, gain_w), 1)
    at_own = pos_r * per_row + pos_c // chip_w == d
    gain_tile = jnp.where(at_own, jnp.tile(gain_pair, (per_row,)).astype(f32)[None, :], 0.0)

    term.append(terms(place, mine, other, gain_tile, w_own, w_other, chip_rows, STREAMS - 1, True))

    st_w = width // STREAMS
    far_up = [(sub * i, sub * ((i + JUMP) % tp)) for i in range(tp)]
    far_down = [(sub * i + 1, sub * ((i - JUMP) % tp) + 1) for i in range(tp)]
    pairs = [*up, *down]
    far_pairs = [*far_up, *far_down]

    class Chain:
        def __init__(self, st, first, last, links):
            self.st, self.at, self.last, self.links = st, first, last, links
            self.value = self.add(None)
            if first == 0:
                self.value = jnp.where(s == 0, self.value, jnp.zeros_like(self.value))

        def add(self, got):
            own = term[self.st][self.at]
            return (own if got is None else got.astype(f32) + own).astype(f16)

        def step(self):
            done = self.at == self.last
            links = self.links if done else pairs
            got = lax.ppermute(self.value, ("tp", "sub"), links)
            if done:
                return got
            self.at += 1
            self.value = self.add(got)

    split = half - JUMP
    chains = [Chain(st, 0, split, far_pairs) for st in range(STREAMS)]
    chains += [Chain(st, split + 1, half - 1, pairs) for st in range(STREAMS)]
    ended = {}
    while len(ended) < len(chains):
        for i, chain in enumerate(chains):
            if i not in ended and (got := chain.step()) is not None:
                ended[i] = got.astype(f32)
    cur = []
    for st in range(STREAMS):
        both = ended[st] + ended[STREAMS + st]
        cur.append(jnp.where(s == 0, both, both + term[st][0]))
    cur_g = cur[-1][:, st_w:].astype(f16)
    cur[-1] = cur[-1][:, :st_w]
    whole = jnp.concatenate(cur, 1)
    own_rows = chip_rows // sub
    upper, lower = whole[:own_rows], whole[own_rows:]
    keep = jnp.where(s == 0, upper, lower)
    give = jnp.where(s == 0, lower, upper).astype(f16)
    hidden = (keep + lax.ppermute(give, "sub", swap).astype(f32)) * (1.0 / sum_up)
    gain_all = (cur_g.astype(f32) + lax.ppermute(cur_g, "sub", swap).astype(f32)).reshape(1, width)

    mean_square = jnp.sum(hidden * hidden, axis=1, keepdims=True) / width
    normed = hidden * lax.rsqrt(mean_square + epsilon) * gain_all
    blocks = normed.reshape(own_rows, width // BLOCK, BLOCK)
    scales = jnp.maximum(jnp.max(jnp.abs(blocks), axis=2), floor_scale).astype(bf16)
    quantized = (blocks / scales.astype(f32)[:, :, None]).reshape(own_rows, width).astype(bf16)
    root = jnp.sqrt(mean_square + epsilon)
    hi = root.astype(f16)
    lo = (root - hi.astype(f32)).astype(f16)
    nb = scales.shape[1]
    small = jnp.concatenate([scales.astype(f16), hi, lo, jnp.zeros((own_rows, BLOCK - 2 - nb), f16)], 1)
    sent = jnp.concatenate([(quantized.astype(f32) * quant_up).astype(f16), small], 1)

    full = lax.all_gather(sent, ("tp", "sub"), axis=0, tiled=True)
    small_all = full[:, width:].astype(f32)
    full_quant = (full[:, :width].astype(f32) * (1.0 / quant_up)).astype(bf16)
    full_scales = small_all[:, :nb].astype(bf16)
    root_all = small_all[:, nb : nb + 1] + small_all[:, nb + 1 : nb + 2]
    q_own = lax.dynamic_slice(full, (zero, me_col), (rows, BLOCK)).astype(f32) * (1.0 / quant_up)
    s_own = lax.dynamic_slice(small_all, (zero, me), (rows, 1))
    new_residual = (q_own * (s_own * root_all) / norm_gain.astype(f32)[None, :]).astype(bf16)
    return full_quant, full_scales, new_residual


def solution(mesh):
    in_specs = (
        P("rep", ("tp", "sub")),
        P(("tp", "sub"), None),
        P("rep", ("tp", "sub")),
        P(("tp", "sub")),
    )
    out_specs = (P("rep", None), P("rep", None), P("rep", ("tp", "sub")))
    return jax.shard_map(
        per_device, mesh=mesh, in_specs=in_specs, out_specs=out_specs, check_vma=False
    )
```
